256 devices in a mesh: gx: 8 (over x, core), gy: 8 (over z), wa: 4 (over y).
Axes of the slice: x: 4, y: 4, z: 8, core: 2. Of those that a mesh axis runs over, the one named last changes fastest.
Arguments:
- velocity: float32 [3, 256, 512, 512], P(None, 'gx', 'gy', 'wa'), may hold values from -70 to 70, as said below
- lengths: int32 [8, 8, 4, 2048], P('gx', 'gy', 'wa'), may hold values from 16 to 128
- destinations: int32 [8, 8, 4, 2048, 1], P('gx', 'gy', 'wa'), may hold values from 0 to 63; in each aligned block of 2048 rows (0 to 2047, 2048 to 4095, ..., all dimensions but the last counted through in order) at most 64 rows name the same one
Outputs:
- received: float32 [64, 4, 3, 64, 64, 128], P(('gx', 'gy'), 'wa')
The draws below stay inside these ranges and needn't reach their ends.
Inputs may be any that keep to these rules, and one draw needn't show every extreme that they name: `velocity`: finite values; the amplitude varies over the grid. `destinations`: in every draw no device sends more than 64 blocks to one writer, and some device sends exactly 64 to one writer.
All inputs are finite; a program needn't handle non-finite values.
Results may differ from the reference program's by a relative error of at most 0.0003.
Values sent between devices are 32-bit elements; how exact they have to be, the bound alone decides.
A program may use at most 128 MiB of HBM per device.

```python
import math
import jax
import jax.numpy as jnp
import numpy as np
from jax import lax

CX = 32
CY = 64
CZ = 128
COMP = 3
BY = 8
BZ = 16
COEF = 128
NBLK = 2048
WRITERS = 64
CAP = 64
NX = 256
NY = 512
NZ = 512
N_GX = 8
N_GY = 8
N_WA = 4


def draw_velocity(key, part):
    xs = jnp.arange(NX, dtype=jnp.float32)[:, None, None] / NX
    ys = jnp.arange(NY, dtype=jnp.float32)[None, :, None] / NY
    noise = jax.random.truncated_normal(key, -6.0, 6.0, (COMP, NX, NY, NZ), jnp.float32)
    amplitude = jnp.exp(jnp.log(10.0) * 0.5 * (xs + ys))
    return amplitude * noise


def place_ends(entries, rng, least, high):
    shape = entries.shape
    spot = [jax.random.randint(jax.random.fold_in(rng, axis), (), 0, shape[axis]) for axis in range(len(shape))]
    entries = entries.at[tuple(spot)].set(least)
    longest = shape.index(max(shape))
    spot[longest] = (spot[longest] + 1) % shape[longest]
    return entries.at[tuple(spot)].set(high)


def shared_out(own_key, own, number, rows, number_of, top, bound, skew):
    sequence = jax.random.permutation(own_key, number_of)
    crowded, usual = load_shares(number_of, rows * top, bound, skew, True), load_shares(number_of, rows * top, bound, skew, False)
    places = jnp.arange(number_of)

    def named(tallies, turn):
        used = int((tallies > 0).sum())
        fixed = max(1, used // 4)
        passed = fixed + (places - fixed + turn * (used - fixed)) % max(1, number_of - fixed)
        return jnp.zeros((number_of,), jnp.int32).at[sequence[jnp.where(places < fixed, places, passed)]].set(jnp.asarray(tallies, jnp.int32))

    tallies = jnp.where(number % 4 == 0, named(crowded, number // 4), named(usual, number - number // 4 - 1))
    mixed = jax.random.permutation(jax.random.fold_in(own, 3), number_of)
    giver, receiver = mixed[0:number_of // 2 * 2:2], mixed[1:number_of // 2 * 2:2]
    room = jnp.minimum(tallies[giver] - 1, bound - tallies[receiver]) // 2
    room = jnp.where((giver == sequence[0]) | (receiver == sequence[0]) | (tallies[receiver] == 0), 0, jnp.maximum(room, 0))
    passed = jax.random.randint(jax.random.fold_in(own, 4), (number_of // 2,), 0, 1 << 20) % (room + 1)
    tallies = tallies.at[giver].add(-passed).at[receiver].add(passed)
    members = jnp.searchsorted(jnp.cumsum(tallies), jnp.arange(rows * top), side="right").astype(jnp.int32)
    grid = members.reshape(top, rows).T
    grid = grid[jax.random.permutation(jax.random.fold_in(own, 1), rows)]
    turn = jax.random.randint(jax.random.fold_in(own, 2), (rows, 1), 0, top)
    return jnp.take_along_axis(grid, (jnp.arange(top)[None, :] + turn) % top, axis=1)


def load_shares(count, total, reach, lean, full):
    weights = [(1 << 20) // math.isqrt(standing ** lean) + 1 for standing in range(1, count + 1)]
    largest = reach if full else min(reach, max(-(-total // count), total * weights[0] // sum(weights)))
    least = 1 if total - largest >= count - 1 else 0
    given, spare = [largest] + [least] * (count - 1), total - largest - least * (count - 1)
    while spare > 0:
        free = [i for i in range(1, count) if given[i] < largest] or [i for i in range(1, count) if given[i] < reach]
        pool, budget = sum([weights[i] for i in free]), spare
        for i in free:
            more = min(reach - given[i], max(1, budget * weights[i] // pool), spare)
            given[i] = given[i] + more
            spare = spare - more
    return np.array(given)


def setup_inputs(seed: int = 0) -> dict:
    key_list = jax.random.split(jax.random.key(seed), 4)
    velocity = draw_velocity(jax.random.fold_in(key_list[3], 71), 0)
    lengths = place_ends(jax.random.randint(key_list[1], (N_GX, N_GY, N_WA, NBLK), 16, COEF + 1), jax.random.fold_in(key_list[1], 1), 16, COEF).astype(jnp.int32)
    destinations_keys = jax.random.split(jax.random.fold_in(key_list[2], 1), N_GX * N_GY * N_WA * NBLK // NBLK)
    destinations_turns = jax.random.permutation(jax.random.fold_in(key_list[2], 3), N_GX * N_GY * N_WA * NBLK // NBLK)
    destinations = jax.vmap(lambda own, number: shared_out(jax.random.fold_in(key_list[2], 2), own, number, NBLK, WRITERS, 1, CAP, 2))(destinations_keys, destinations_turns).reshape((N_GX, N_GY, N_WA, NBLK, 1))
    return dict(velocity=velocity, lengths=lengths, destinations=destinations)


def dct_table(count):
    freqs = jnp.arange(count, dtype=jnp.float32)[:, None]
    points = jnp.arange(count, dtype=jnp.float32)[None, :]
    table = jnp.cos(jnp.pi * (points + 0.5) * freqs / count) * jnp.sqrt(2.0 / count)
    return jnp.where(freqs == 0.0, table * jnp.sqrt(0.5), table)

def curl_field(padded):

    def along_x(component):
        return (padded[component, 2:, 1:-1, 1:-1] - padded[component, :-2, 1:-1, 1:-1]) * 0.5

    def along_y(component):
        return (padded[component, 1:-1, 2:, 1:-1] - padded[component, 1:-1, :-2, 1:-1]) * 0.5

    def along_z(component):
        return (padded[component, 1:-1, 1:-1, 2:] - padded[component, 1:-1, 1:-1, :-2]) * 0.5
    first = along_y(2) - along_z(1)
    second = along_z(0) - along_x(2)
    third = along_x(1) - along_y(0)
    return jnp.stack([first, second, third])

def place_blocks(scaled, lens, targets):
    onehot = (targets[:, None] == jnp.arange(WRITERS, dtype=jnp.int32)[None, :]).astype(jnp.int32)
    before = jnp.cumsum(onehot, axis=0) - onehot
    ranking = lax.optimization_barrier(jnp.sum(before * onehot, axis=1))
    slot_index = (targets * CAP + ranking).astype(jnp.int32)
    buffer = jnp.zeros((WRITERS * CAP, COMP, COEF), jnp.float32)
    buffer = buffer.at[slot_index].set(scaled)
    return buffer.reshape(WRITERS, CAP, COMP, COEF)

def reference(velocity, lengths, destinations):
    padded = jnp.pad(velocity, ((0, 0), (1, 1), (1, 1), (1, 1)), mode='wrap')
    curl = curl_field(padded)
    total = jnp.sum(curl * curl)
    rms = jnp.sqrt(total / (COMP * NX * NY * NZ) + 1e-06)
    kron_table = jnp.kron(dct_table(BY), dct_table(BZ))
    grouped = curl.reshape(COMP, N_GX, CX, N_GY, CY // BY, BY, N_WA, CZ // BZ, BZ)
    grouped = grouped.transpose(1, 3, 6, 2, 4, 7, 0, 5, 8)
    blocks = grouped.reshape(-1, COEF)
    coeffs = jnp.dot(blocks, kron_table.T, precision=lax.Precision.HIGHEST, preferred_element_type=jnp.float32)
    coeffs = coeffs.reshape(N_GX * N_GY * N_WA, NBLK, COMP, COEF)
    freqs = jnp.arange(COEF, dtype=jnp.int32)
    lens = lengths.reshape(N_GX * N_GY * N_WA, NBLK)
    keep = (freqs[None, None, None, :] < lens[:, :, None, None]).astype(jnp.float32)
    scaled = coeffs * keep / rms
    targets = destinations.reshape(N_GX * N_GY * N_WA, NBLK)
    buffers = jax.vmap(place_blocks)(scaled, lens, targets)
    buffers = buffers.reshape(WRITERS, N_WA, WRITERS, CAP, COMP, COEF)
    return buffers.transpose(2, 1, 4, 0, 3, 5)
```

```python
import functools

import jax
import jax.numpy as jnp
from jax import lax
from jax.experimental import pallas as pl
from jax.experimental.pallas import tpu as pltpu
from jax.sharding import PartitionSpec as P

BY = 8
BZ = 16
COMP = 3
LANES = 128
MESH = pl.DeviceIdType.MESH


def dct_table(count):
    freqs = jnp.arange(count, dtype=jnp.float32)[:, None]
    points = jnp.arange(count, dtype=jnp.float32)[None, :]
    table = jnp.cos(jnp.pi * (points + 0.5) * freqs / count) * jnp.sqrt(2.0 / count)
    return jnp.where(freqs == 0.0, table * jnp.sqrt(0.5), table)


def split(value):
    high = value.astype(jnp.bfloat16)
    low = (value - high.astype(jnp.float32)).astype(jnp.bfloat16)
    return high, low


def dot(a, b):
    return jnp.dot(a, b, preferred_element_type=jnp.float32)


def iota(shape, dim):
    return lax.broadcasted_iota(jnp.int32, shape, dim)


def table_kernel(writers, cap, dest_ref, lens_ref, slots_ref, keep_ref):
    groups = dest_ref.shape[0]
    nblk = groups * LANES
    square = (LANES, LANES)
    upper = (iota(square, 0) < iota(square, 1)).astype(jnp.bfloat16)
    diagonal = iota(square, 0) == iota(square, 1)
    ones = jnp.ones(square, jnp.bfloat16)
    freqs = iota(square, 1).astype(jnp.float32)
    rows_w = iota((writers, LANES), 0)
    rows_s = iota((cap, LANES), 0).astype(jnp.float32)
    lane = iota((1, LANES), 1)
    count = jnp.zeros((writers, 1), jnp.float32)
    high = jnp.zeros((writers, cap), jnp.float32)
    low = jnp.zeros((writers, cap), jnp.float32)
    across = (((1,), (1,)), ((), ()))
    for group in range(groups):
        named = rows_w == dest_ref[pl.ds(group, 1), :]
        one = named.astype(jnp.float32)
        one_b = one.astype(jnp.bfloat16)
        before = dot(one_b, upper) + count
        rank = jnp.sum(one * before, axis=0, keepdims=True)
        at_slot = rows_s == rank
        number = lane + (group * LANES + 1)
        top = jnp.where(at_slot, (number // 64).astype(jnp.float32), 0.0).astype(jnp.bfloat16)
        rest = jnp.where(at_slot, (number % 64).astype(jnp.float32), 0.0).astype(jnp.bfloat16)
        high += lax.dot_general(one_b, top, across, preferred_element_type=jnp.float32)
        low += lax.dot_general(one_b, rest, across, preferred_element_type=jnp.float32)
        count += jnp.sum(one, axis=1, keepdims=True)
        lens = lens_ref[pl.ds(group, 1), :].astype(jnp.float32)
        spread = jnp.where(diagonal, jnp.broadcast_to(lens, square), 0.0).astype(jnp.bfloat16)
        keep_ref[pl.ds(group * LANES, LANES), :] = (freqs < dot(spread, ones)).astype(jnp.float32)
    code = (high * 64.0 + low).astype(jnp.int32)
    slots_ref[...] = jnp.where(code == 0, nblk, code - 1)


def exchange_kernel(
    sizes, velocity, slots, keep, table, received, total,
    field, y_out, y_in, z_out, z_in, turned, coeffs, rows, part, parts, plane_sum, plane_sums,
    in_sem, halo_send, halo_recv, row_send, row_recv, own_sem, part_send, part_recv, sum_send, sum_recv,
):
    n_gx, n_gy, n_wa, cells_x, cells_y, nblk, cap = sizes
    writers = n_gx * n_gy
    tiles_y = cells_y // 8
    gx, gy, wa = lax.axis_index("gx"), lax.axis_index("gy"), lax.axis_index("wa")
    me = gx * n_gy + gy

    def writer(w):
        return (w // n_gy, lax.rem(w, n_gy), wa)

    barrier = pltpu.get_barrier_semaphore()

    def greet(i, carry):
        pl.semaphore_signal(
            barrier, inc=1, device_id=writer(lax.rem(me + i, writers)), device_id_type=MESH
        )
        return carry

    lax.fori_loop(1, writers, greet, 0)
    for k in range(1, n_wa):
        pl.semaphore_signal(
            barrier, inc=1, device_id=(gx, gy, lax.rem(wa + k, n_wa)), device_id_type=MESH
        )

    loads = [
        pltpu.make_async_copy(
            velocity.at[c], field.at[c, pl.ds(cells_y, cells_x * cells_y)], in_sem.at[c]
        )
        for c in range(COMP)
    ]
    for load in loads:
        load.start()
    for load in loads:
        load.wait()

    lane = iota((8, LANES), 1)

    def pack_y(x, carry):
        for j, c in enumerate((0, 2)):
            first = field[c, pl.ds(cells_y + x * cells_y, 8), :]
            last = field[c, pl.ds(2 * cells_y - 8 + x * cells_y, 8), :]
            y_out[0, j, pl.ds(x, 1), :] = first[0:1]
            y_out[1, j, pl.ds(x, 1), :] = last[7:8]
        return carry

    lax.fori_loop(0, cells_x, pack_y, 0)

    packs = cells_x * tiles_y // LANES

    def pack_z(k, carry):
        out = []
        for j in range(2):
            for g in range(packs):
                tile = field[j, pl.ds(cells_y + (g * LANES + k) * 8, 8), :]
                low, high = carry[len(out)]
                low = jnp.where(lane == k, pltpu.roll(tile, k, 1), low)
                high = jnp.where(lane == k, pltpu.roll(tile, lax.rem(k + 1, LANES), 1), high)
                out.append((low, high))
        return tuple(out)

    zero = jnp.zeros((8, LANES), jnp.float32)
    packed = lax.fori_loop(0, LANES, pack_z, tuple((zero, zero) for _ in range(2 * packs)))
    for q, (low, high) in enumerate(packed):
        z_out[0, q] = low
        z_out[1, q] = high

    pl.semaphore_wait(barrier, writers - 1 + n_wa - 1)

    x_up = (lax.rem(gx + 1, n_gx), gy, wa)
    x_down = (lax.rem(gx + n_gx - 1, n_gx), gy, wa)
    y_up = (gx, lax.rem(gy + 1, n_gy), wa)
    y_down = (gx, lax.rem(gy + n_gy - 1, n_gy), wa)
    z_up = (gx, gy, lax.rem(wa + 1, n_wa))
    z_down = (gx, gy, lax.rem(wa + n_wa - 1, n_wa))
    faces = [
        (field.at[pl.ds(1, 2), pl.ds(cells_y, cells_y)],
         field.at[pl.ds(1, 2), pl.ds((cells_x + 1) * cells_y, cells_y)], x_down),
        (field.at[pl.ds(1, 2), pl.ds(cells_x * cells_y, cells_y)],
         field.at[pl.ds(1, 2), pl.ds(0, cells_y)], x_up),
        (y_out.at[0], y_in.at[0], y_down),
        (y_out.at[1], y_in.at[1], y_up),
        (z_out.at[0], z_in.at[0], z_down),
        (z_out.at[1], z_in.at[1], z_up),
    ]
    halos = [
        pltpu.make_async_remote_copy(
            src_ref=source, dst_ref=target, send_sem=halo_send.at[k], recv_sem=halo_recv.at[k],
            device_id=peer, device_id_type=MESH,
        )
        for k, (source, target, peer) in enumerate(faces)
    ]
    for halo in halos:
        halo.start()
    for halo in halos:
        halo.wait()

    row = iota((cells_y, LANES), 0)
    column = iota((cells_y, LANES), 1)
    group = column // BZ
    lower = []
    for step in (4, 2, 1):
        row_bit = (row // step) % 2
        group_bit = (group // step) % 2
        lower.append((step, (row_bit == 0) & (group_bit == 1), (row_bit == 1) & (group_bit == 0)))

    def turn(plane):
        for step, up, down in lower:
            ahead = pltpu.roll(pltpu.roll(plane, BZ * step, 1), cells_y - step, 0)
            behind = pltpu.roll(pltpu.roll(plane, LANES - BZ * step, 1), step, 0)
            plane = jnp.where(up, ahead, jnp.where(down, behind, plane))
        return plane

    def along_x(c, x):
        after = field[c, pl.ds((x + 2) * cells_y, cells_y), :]
        return after - field[c, pl.ds(x * cells_y, cells_y), :]

    def along_y(plane, j, x):
        after = jnp.where(row == cells_y - 1, y_in[0, j, pl.ds(x, 1), :], pltpu.roll(plane, cells_y - 1, 0))
        before = jnp.where(row == 0, y_in[1, j, pl.ds(x, 1), :], pltpu.roll(plane, 1, 0))
        return after - before

    def along_z(plane, j, x):
        per = LANES // tiles_y
        q = j * packs + x // per
        base = lax.rem(x, per) * tiles_y
        nexts, lasts = z_in[0, q], z_in[1, q]
        after = jnp.concatenate(
            [pltpu.roll(nexts, LANES - 1 - base - t, 1) for t in range(tiles_y)], axis=0
        )
        before = jnp.concatenate(
            [pltpu.roll(lasts, lax.rem(LANES - base - t, LANES), 1) for t in range(tiles_y)], axis=0
        )
        after = jnp.where(column == LANES - 1, after, pltpu.roll(plane, LANES - 1, 1))
        before = jnp.where(column == 0, before, pltpu.roll(plane, 1, 1))
        return after - before

    def curl(x, square):
        here = pl.ds((x + 1) * cells_y, cells_y)
        u, v, w = field[0, here, :], field[1, here, :], field[2, here, :]
        first = (along_y(w, 1, x) - along_z(v, 1, x)) * 0.5
        second = (along_z(u, 0, x) - along_x(2, x)) * 0.5
        third = (along_x(1, x) - along_y(u, 0, x)) * 0.5
        for c, plane in enumerate((first, second, third)):
            turned[c, pl.ds(x * cells_y, cells_y), :] = turn(plane)
            square += plane * plane
        return square

    square = lax.fori_loop(0, cells_x, curl, jnp.zeros((cells_y, LANES), jnp.float32))
    part[...] = jnp.sum(square.reshape(tiles_y, 8, LANES), axis=0)
    parts[pl.ds(me, 1)] = part[...][None]

    def part_copy(i, peer, slot):
        return pltpu.make_async_remote_copy(
            src_ref=part, dst_ref=parts.at[slot], send_sem=part_send.at[i],
            recv_sem=part_recv.at[i], device_id=writer(peer), device_id_type=MESH,
        )

    def part_start(i, carry):
        part_copy(i, lax.rem(me + i, writers), me).start()
        return carry

    lax.fori_loop(1, writers, part_start, 0)

    coeffs[pl.ds(nblk, 8), :] = zero
    chunk = 2 * LANES

    def row_copy(c, i, peer, slot):
        return pltpu.make_async_remote_copy(
            src_ref=rows.at[c, peer], dst_ref=received.at[c, slot], send_sem=row_send.at[c, i],
            recv_sem=row_recv.at[c, i], device_id=writer(peer), device_id_type=MESH,
        )

    def own_copy(c):
        return pltpu.make_async_copy(rows.at[c, me], received.at[c, me], own_sem.at[c])

    for c in range(COMP):

        def transform(k, carry):
            at = pl.ds(k * chunk, chunk)
            high, low = split(turned[c, at, :])
            value = dot(high, table[0]) + (dot(low, table[0]) + dot(high, table[1]))
            coeffs[at, :] = value * keep[at, :]
            return carry

        lax.fori_loop(0, nblk // chunk, transform, 0)

        def gather(i):
            w = lax.rem(me + i, writers)
            for s in range(cap):
                rows[c, w, pl.ds(s, 1), :] = coeffs[pl.ds(slots[w, s], 1), :]

        def send(i):
            row_copy(c, i, lax.rem(me + i, writers), me).start()

        gather(1)

        def step(i, carry):
            gather(i)
            send(i - 1)
            return carry

        lax.fori_loop(2, writers, step, 0)
        gather(0)
        send(writers - 1)
        own_copy(c).start()

        if c == 0:

            def part_wait(i, carry):
                part_copy(i, lax.rem(me + i, writers), lax.rem(me + writers - i, writers)).wait()
                return carry

            lax.fori_loop(1, writers, part_wait, 0)
            plane_sum[...] = jnp.sum(parts[...], axis=0)
            plane_sums[pl.ds(wa, 1)] = plane_sum[...][None]
            sums = [
                pltpu.make_async_remote_copy(
                    src_ref=plane_sum, dst_ref=plane_sums.at[wa], send_sem=sum_send.at[k],
                    recv_sem=sum_recv.at[k], device_id=(gx, gy, lax.rem(wa + k, n_wa)),
                    device_id_type=MESH,
                )
                for k in range(1, n_wa)
            ]
            for copy in sums:
                copy.start()

    for k in range(1, n_wa):
        pltpu.make_async_remote_copy(
            src_ref=plane_sum, dst_ref=plane_sums.at[lax.rem(wa + n_wa - k, n_wa)],
            send_sem=sum_send.at[k], recv_sem=sum_recv.at[k],
            device_id=(gx, gy, lax.rem(wa + k, n_wa)), device_id_type=MESH,
        ).wait()
    total[...] = jnp.sum(plane_sums[...], axis=0)

    for c in range(COMP):
        own_copy(c).wait()

        def row_wait(i, carry):
            row_copy(c, i, lax.rem(me + i, writers), lax.rem(me + writers - i, writers)).wait()
            return carry

        lax.fori_loop(1, writers, row_wait, 0)


def local(n_gx, n_gy, n_wa, velocity, lengths, destinations):
    comps, cells_x, cells_y, cells_z = velocity.shape
    nblk = lengths.size
    writers = n_gx * n_gy
    cap = max(2, 2 * nblk // writers)
    whole = pl.BlockSpec(memory_space=pltpu.VMEM)
    slots, keep = pl.pallas_call(
        functools.partial(table_kernel, writers, cap),
        out_shape=(
            jax.ShapeDtypeStruct((writers, cap), jnp.int32),
            jax.ShapeDtypeStruct((nblk, LANES), jnp.float32),
        ),
        in_specs=[whole, whole],
        out_specs=(whole, whole),
    )(destinations.reshape(nblk // LANES, LANES), lengths.reshape(nblk // LANES, LANES))
    exact = jnp.kron(dct_table(BY), dct_table(BZ)).T
    high = lax.reduce_precision(exact, 8, 7)
    table = jnp.stack([high, exact - high]).astype(jnp.bfloat16)
    sizes = (n_gx, n_gy, n_wa, cells_x, cells_y, nblk, cap)
    f32 = jnp.float32
    packs = cells_x * cells_y // 8 // LANES
    dma = pltpu.SemaphoreType.DMA
    received, total = pl.pallas_call(
        functools.partial(exchange_kernel, sizes),
        out_shape=(
            jax.ShapeDtypeStruct((comps, writers, cap, LANES), f32),
            jax.ShapeDtypeStruct((8, LANES), f32),
        ),
        in_specs=[
            pl.BlockSpec(memory_space=pl.ANY),
            pl.BlockSpec(memory_space=pltpu.SMEM),
            whole,
            whole,
        ],
        out_specs=(pl.BlockSpec(memory_space=pl.ANY), whole),
        scratch_shapes=[
            pltpu.VMEM((comps, (cells_x + 2) * cells_y, LANES), f32),
            pltpu.VMEM((2, 2, cells_x, LANES), f32),
            pltpu.VMEM((2, 2, cells_x, LANES), f32),
            pltpu.VMEM((2, 2 * packs, 8, LANES), f32),
            pltpu.VMEM((2, 2 * packs, 8, LANES), f32),
            pltpu.VMEM((comps, nblk, LANES), f32),
            pltpu.VMEM((nblk + 8, LANES), f32),
            pltpu.VMEM((comps, writers, cap, LANES), f32),
            pltpu.VMEM((8, LANES), f32),
            pltpu.VMEM((writers, 8, LANES), f32),
            pltpu.VMEM((8, LANES), f32),
            pltpu.VMEM((n_wa, 8, LANES), f32),
            dma((comps,)),
            dma((6,)),
            dma((6,)),
            dma((comps, writers)),
            dma((comps, writers)),
            dma((comps,)),
            dma((writers,)),
            dma((writers,)),
            dma((n_wa,)),
            dma((n_wa,)),
        ],
        compiler_params=pltpu.CompilerParams(
            collective_id=0, has_side_effects=True, vmem_limit_bytes=32 * 2**20
        ),
    )(velocity.reshape(comps, cells_x * cells_y, cells_z), slots, keep, table)
    every = velocity.size * n_gx * n_gy * n_wa
    rms = jnp.sqrt(jnp.sum(total) / every + 1e-06)
    return (received * (1.0 / rms)).reshape(1, 1, comps, writers, cap, LANES)


def solution(mesh):
    n_gx, n_gy, n_wa = mesh.shape["gx"], mesh.shape["gy"], mesh.shape["wa"]
    return jax.shard_map(
        functools.partial(local, n_gx, n_gy, n_wa),
        mesh=mesh,
        in_specs=(
            P(None, "gx", "gy", "wa"),
            P("gx", "gy", "wa", None),
            P("gx", "gy", "wa", None, None),
        ),
        out_specs=P(("gx", "gy"), "wa", None, None, None, None),
        check_vma=False,
    )
```

```python
import functools

import jax
import jax.numpy as jnp
from jax import lax
from jax.experimental import pallas as pl
from jax.experimental.pallas import tpu as pltpu
from jax.sharding import PartitionSpec as P

BY = 8
BZ = 16
COMP = 3
LANES = 128
MESH = pl.DeviceIdType.MESH


def dct_table(count):
    freqs = jnp.arange(count, dtype=jnp.float32)[:, None]
    points = jnp.arange(count, dtype=jnp.float32)[None, :]
    table = jnp.cos(jnp.pi * (points + 0.5) * freqs / count) * jnp.sqrt(2.0 / count)
    return jnp.where(freqs == 0.0, table * jnp.sqrt(0.5), table)


def split(value):
    high = value.astype(jnp.bfloat16)
    low = (value - high.astype(jnp.float32)).astype(jnp.bfloat16)
    return high, low


def dot(a, b):
    return jnp.dot(a, b, preferred_element_type=jnp.float32)


def iota(shape, dim):
    return lax.broadcasted_iota(jnp.int32, shape, dim)


def turned_row(block):
    return block // 64 * 64 + block % 8 * 8 + block // 8 % 8


def make_table(writers, cap, dest_ref, lens_ref, slots_ref, keep_ref):
    groups = dest_ref.shape[0]
    nblk = groups * LANES
    square = (LANES, LANES)
    upper = (iota(square, 0) < iota(square, 1)).astype(jnp.bfloat16)
    diagonal = iota(square, 0) == turned_row(iota(square, 1))
    ones = jnp.ones(square, jnp.bfloat16)
    freqs = iota(square, 1).astype(jnp.float32)
    rows_w = iota((writers, LANES), 0)
    rows_s = iota((cap, LANES), 0).astype(jnp.float32)
    lane = iota((1, LANES), 1)
    count = jnp.zeros((writers, 1), jnp.float32)
    high = jnp.zeros((writers, cap), jnp.float32)
    low = jnp.zeros((writers, cap), jnp.float32)
    across = (((1,), (1,)), ((), ()))
    for group in range(groups):
        named = rows_w == dest_ref[pl.ds(group, 1), :]
        one = named.astype(jnp.float32)
        one_b = one.astype(jnp.bfloat16)
        before = dot(one_b, upper) + count
        rank = jnp.sum(one * before, axis=0, keepdims=True)
        at_slot = rows_s == rank
        number = turned_row(lane) + (group * LANES + 1)
        top = jnp.where(at_slot, (number // 64).astype(jnp.float32), 0.0).astype(jnp.bfloat16)
        rest = jnp.where(at_slot, (number % 64).astype(jnp.float32), 0.0).astype(jnp.bfloat16)
        high += lax.dot_general(one_b, top, across, preferred_element_type=jnp.float32)
        low += lax.dot_general(one_b, rest, across, preferred_element_type=jnp.float32)
        count += jnp.sum(one, axis=1, keepdims=True)
        lens = lens_ref[pl.ds(group, 1), :].astype(jnp.float32)
        spread = jnp.where(diagonal, jnp.broadcast_to(lens, square), 0.0).astype(jnp.bfloat16)
        keep_ref[pl.ds(group * LANES, LANES), :] = (freqs < dot(spread, ones)).astype(jnp.float32)
    code = (high * 64.0 + low).astype(jnp.int32)
    slots_ref[...] = jnp.clip(jnp.where(code == 0, nblk, code - 1), 0, nblk)


def exchange_kernel(
    sizes, field, dest, lens, table, result,
    x_in, y_out, y_in, z_out, z_in, turned, coeffs, rows, received, keep, slots_v, slots,
    part, parts, plane_sum, plane_sums,
    halo_send, halo_recv, row_send, row_recv, own_sem, out_sem, slot_sem,
    part_send, part_recv, sum_send, sum_recv,
):
    n_gx, n_gy, n_wa, cells_x, cells_y, nblk, cap = sizes
    writers = n_gx * n_gy
    tiles_y = cells_y // 8
    gx, gy, wa = lax.axis_index("gx"), lax.axis_index("gy"), lax.axis_index("wa")
    me = gx * n_gy + gy

    def writer(w):
        return (w // n_gy, lax.rem(w, n_gy), wa)

    barrier = pltpu.get_barrier_semaphore()

    def greet(i, carry):
        pl.semaphore_signal(
            barrier, inc=1, device_id=writer(lax.rem(me + i, writers)), device_id_type=MESH
        )
        return carry

    lax.fori_loop(1, writers, greet, 0)
    for k in range(1, n_wa):
        pl.semaphore_signal(
            barrier, inc=1, device_id=(gx, gy, lax.rem(wa + k, n_wa)), device_id_type=MESH
        )

    lane = iota((8, LANES), 1)
    sub = iota((8, LANES), 0)
    zero = jnp.zeros((8, LANES), jnp.float32)
    packs = cells_x * 8 // LANES
    per = cells_x // packs

    def tile(c, x, y):
        return field[c, pl.ds(x * cells_y + y, tiles_y, stride=8), :]

    def pack_y(c, j):
        def pack(x, carry):
            y_out[0, j, pl.ds(x, 1), :] = field[c, pl.ds(x * cells_y, 1), :]
            y_out[1, j, pl.ds(x, 1), :] = field[c, pl.ds((x + 1) * cells_y - 1, 1), :]
            return carry

        lax.fori_loop(0, cells_x, pack, 0)

    def pack_z(c, j):
        for g in range(packs):

            def pack(step, carry):
                low, high = carry
                for x, y in [(x, y) for x in range(2) for y in range(8)]:
                    k = (step * 2 + x) * 8 + y
                    here = tile(c, g * per + step * 2 + x, y)
                    low = jnp.where(lane == k, pltpu.roll(here, k, 1), low)
                    high = jnp.where(lane == k, pltpu.roll(here, lax.rem(k + 1, LANES), 1), high)
                return low, high

            low, high = lax.fori_loop(0, per // 2, pack, (zero, zero))
            z_out[0, j, g] = low
            z_out[1, j, g] = high

    x_up = (lax.rem(gx + 1, n_gx), gy, wa)
    x_down = (lax.rem(gx + n_gx - 1, n_gx), gy, wa)
    y_up = (gx, lax.rem(gy + 1, n_gy), wa)
    y_down = (gx, lax.rem(gy + n_gy - 1, n_gy), wa)
    z_up = (gx, gy, lax.rem(wa + 1, n_wa))
    z_down = (gx, gy, lax.rem(wa + n_wa - 1, n_wa))
    faces = [
        (z_out.at[0, 1], z_in.at[0, 1], z_down),
        (z_out.at[1, 1], z_in.at[1, 1], z_up),
        (y_out.at[0, 1], y_in.at[0, 1], y_down),
        (y_out.at[1, 1], y_in.at[1, 1], y_up),
        (z_out.at[0, 0], z_in.at[0, 0], z_down),
        (z_out.at[1, 0], z_in.at[1, 0], z_up),
        (y_out.at[0, 0], y_in.at[0, 0], y_down),
        (y_out.at[1, 0], y_in.at[1, 0], y_up),
        (field.at[pl.ds(1, 2), pl.ds(0, cells_y)], x_in.at[0], x_down),
        (field.at[pl.ds(1, 2), pl.ds((cells_x - 1) * cells_y, cells_y)], x_in.at[1], x_up),
    ]
    halos = [
        pltpu.make_async_remote_copy(
            src_ref=source, dst_ref=target, send_sem=halo_send.at[k], recv_sem=halo_recv.at[k],
            device_id=peer, device_id_type=MESH,
        )
        for k, (source, target, peer) in enumerate(faces)
    ]

    pack_z(1, 1)
    pack_y(2, 1)
    pack_z(0, 0)
    pack_y(0, 0)
    make_table(writers, cap, dest, lens, slots_v, keep)
    slot_copy = pltpu.make_async_copy(slots_v, slots, slot_sem)
    slot_copy.start()
    pl.semaphore_wait(barrier, writers - 1 + n_wa - 1)
    for halo in halos:
        halo.start()
    coeffs[pl.ds(nblk, 8), :] = zero

    group = lane // BZ

    def turn(tiles):
        for step in (4, 2, 1):
            bit = (group // step) % 2 == 1
            out = list(tiles)
            for a in range(8):
                if a & step == 0:
                    b = a | step
                    out[a] = jnp.where(bit, pltpu.roll(tiles[b], BZ * step, 1), tiles[a])
                    out[b] = jnp.where(bit, tiles[b], pltpu.roll(tiles[a], LANES - BZ * step, 1))
            tiles = out
        return tiles

    def along_x(c, x, edge):
        def near(at, d):
            if edge == d:
                return [x_in[d, c - 1, pl.ds(y, tiles_y, stride=8), :] for y in range(8)]
            return [tile(c, at, y) for y in range(8)]

        return [a - b for a, b in zip(near(x + 1, 0), near(x - 1, 1))]

    def along_y(c, j, x):
        here = [tile(c, x, y) for y in range(8)]
        after = jnp.where(sub == tiles_y - 1, y_in[0, j, pl.ds(x, 1), :], pltpu.roll(here[0], tiles_y - 1, 0))
        before = jnp.where(sub == 0, y_in[1, j, pl.ds(x, 1), :], pltpu.roll(here[7], 1, 0))
        return [a - b for a, b in zip(here[1:] + [after], [before] + here[:-1])]

    def along_z(c, j, x):
        nexts, lasts = z_in[0, j, x // per], z_in[1, j, x // per]
        out = []
        for y in range(8):
            k = lax.rem(x, per) * 8 + y
            here = tile(c, x, y)
            after = jnp.where(
                lane == LANES - 1, pltpu.roll(nexts, LANES - 1 - k, 1), pltpu.roll(here, LANES - 1, 1)
            )
            before = jnp.where(
                lane == 0, pltpu.roll(lasts, lax.rem(LANES - k, LANES), 1), pltpu.roll(here, 1, 1)
            )
            out.append(after - before)
        return out

    def curl(c, square):
        def at(x, square, edge=None):
            if c == 0:
                pairs = zip(along_y(2, 1, x), along_z(1, 1, x))
            elif c == 1:
                pairs = zip(along_z(0, 0, x), along_x(2, x, edge))
            else:
                pairs = zip(along_x(1, x, edge), along_y(0, 0, x))
            tiles = [(a - b) * 0.5 for a, b in pairs]
            for t in tiles:
                square += t * t
            for z, t in enumerate(turn(tiles)):
                turned[c, pl.ds(x * cells_y + z * tiles_y, tiles_y), :] = t
            return square

        if c == 0:
            return lax.fori_loop(0, cells_x // 2, lambda i, q: at(2 * i + 1, at(2 * i, q)), square)
        square = at(0, square, 1)
        square = lax.fori_loop(1, cells_x - 1, at, square)
        return at(cells_x - 1, square, 0)

    chunk = 2 * LANES

    def row_copy(c, i, slot):
        peer = lax.rem(me + i, writers)
        return pltpu.make_async_remote_copy(
            src_ref=rows.at[c, peer], dst_ref=received.at[c, slot], send_sem=row_send.at[c, i],
            recv_sem=row_recv.at[c, i], device_id=writer(peer), device_id_type=MESH,
        )

    def own_copy(c):
        return pltpu.make_async_copy(rows.at[c, me], received.at[c, me], own_sem.at[c])

    def deliver(c):
        def transform(k, carry):
            at = pl.ds(k * chunk, chunk)
            high, low = split(turned[c, at, :])
            value = dot(high, table[0]) + (dot(low, table[0]) + dot(high, table[1]))
            coeffs[at, :] = value * keep[at, :]
            return carry

        lax.fori_loop(0, nblk // chunk, transform, 0)

        def gather(i):
            w = lax.rem(me + i, writers)
            for s in range(cap):
                rows[c, w, pl.ds(s, 1), :] = coeffs[pl.ds(slots[w, s], 1), :]

        gather(1)

        def step(i, carry):
            gather(i)
            row_copy(c, i - 1, me).start()
            return carry

        lax.fori_loop(2, writers, step, 0)
        gather(0)
        row_copy(c, writers - 1, me).start()
        own_copy(c).start()

    def part_copy(i, slot):
        return pltpu.make_async_remote_copy(
            src_ref=part, dst_ref=parts.at[slot], send_sem=part_send.at[i],
            recv_sem=part_recv.at[i], device_id=writer(lax.rem(me + i, writers)),
            device_id_type=MESH,
        )

    def sum_copy(k, slot):
        return pltpu.make_async_remote_copy(
            src_ref=plane_sum, dst_ref=plane_sums.at[slot], send_sem=sum_send.at[k],
            recv_sem=sum_recv.at[k], device_id=(gx, gy, lax.rem(wa + k, n_wa)),
            device_id_type=MESH,
        )

    for halo in halos[:4]:
        halo.wait()
    square = curl(0, zero)
    slot_copy.wait()
    deliver(0)
    for halo in halos[4:]:
        halo.wait()
    square = curl(2, curl(1, square))
    part[...] = square
    parts[pl.ds(me, 1)] = part[...][None]

    def part_start(i, carry):
        part_copy(i, me).start()
        return carry

    lax.fori_loop(1, writers, part_start, 0)
    deliver(1)
    deliver(2)

    def part_wait(i, carry):
        part_copy(i, lax.rem(me + writers - i, writers)).wait()
        return carry

    lax.fori_loop(1, writers, part_wait, 0)
    plane_sum[...] = jnp.sum(parts[...], axis=0)
    plane_sums[pl.ds(wa, 1)] = plane_sum[...][None]
    for k in range(1, n_wa):
        sum_copy(k, wa).start()
    for k in range(1, n_wa):
        sum_copy(k, lax.rem(wa + n_wa - k, n_wa)).wait()
    total = jnp.sum(plane_sums[...], axis=0)
    total = jnp.sum(jnp.sum(total, axis=0, keepdims=True), axis=1, keepdims=True)
    every = COMP * cells_x * cells_y * LANES * writers * n_wa
    scale = 1.0 / jnp.sqrt(total / every + 1e-06)
    scale = jnp.broadcast_to(jnp.broadcast_to(scale, (1, LANES)), (cap, LANES))

    for c in range(COMP):
        own_copy(c).wait()

        def row_wait(i, carry):
            row_copy(c, i, lax.rem(me + writers - i, writers)).wait()
            return carry

        lax.fori_loop(1, writers, row_wait, 0)

        def rescale(s, carry):
            received[c, s] = received[c, s] * scale
            return carry

        lax.fori_loop(0, writers, rescale, 0)
        pltpu.make_async_copy(received.at[c], result.at[c], out_sem.at[c]).start()
    for c in range(COMP):
        pltpu.make_async_copy(received.at[c], result.at[c], out_sem.at[c]).wait()


def local(n_gx, n_gy, n_wa, velocity, lengths, destinations):
    comps, cells_x, cells_y, cells_z = velocity.shape
    nblk = lengths.size
    writers = n_gx * n_gy
    cap = max(2, 2 * nblk // writers)
    whole = pl.BlockSpec(memory_space=pltpu.VMEM)
    exact = jnp.kron(dct_table(BY), dct_table(BZ)).T
    high = lax.reduce_precision(exact, 8, 7)
    table = jnp.stack([high, exact - high]).astype(jnp.bfloat16)
    sizes = (n_gx, n_gy, n_wa, cells_x, cells_y, nblk, cap)
    f32 = jnp.float32
    packs = cells_x * cells_y // 8 // LANES
    dma = pltpu.SemaphoreType.DMA
    result = pl.pallas_call(
        functools.partial(exchange_kernel, sizes),
        out_shape=jax.ShapeDtypeStruct((comps, writers, cap, LANES), f32),
        in_specs=[whole, whole, whole, whole],
        out_specs=pl.BlockSpec(memory_space=pl.ANY),
        scratch_shapes=[
            pltpu.VMEM((2, 2, cells_y, LANES), f32),
            pltpu.VMEM((2, 2, cells_x, LANES), f32),
            pltpu.VMEM((2, 2, cells_x, LANES), f32),
            pltpu.VMEM((2, 2, packs, 8, LANES), f32),
            pltpu.VMEM((2, 2, packs, 8, LANES), f32),
            pltpu.VMEM((comps, nblk, LANES), f32),
            pltpu.VMEM((nblk + 8, LANES), f32),
            pltpu.VMEM((comps, writers, cap, LANES), f32),
            pltpu.VMEM((comps, writers, cap, LANES), f32),
            pltpu.VMEM((nblk, LANES), f32),
            pltpu.VMEM((writers, cap), jnp.int32),
            pltpu.SMEM((writers, cap), jnp.int32),
            pltpu.VMEM((8, LANES), f32),
            pltpu.VMEM((writers, 8, LANES), f32),
            pltpu.VMEM((8, LANES), f32),
            pltpu.VMEM((n_wa, 8, LANES), f32),
            dma((10,)),
            dma((10,)),
            dma((comps, writers)),
            dma((comps, writers)),
            dma((comps,)),
            dma((comps,)),
            dma,
            dma((writers,)),
            dma((writers,)),
            dma((n_wa,)),
            dma((n_wa,)),
        ],
        compiler_params=pltpu.CompilerParams(
            collective_id=0, has_side_effects=True, vmem_limit_bytes=40 * 2**20
        ),
    )(
        velocity.reshape(comps, cells_x * cells_y, cells_z),
        destinations.reshape(nblk // LANES, LANES),
        lengths.reshape(nblk // LANES, LANES),
        table,
    )
    return result.reshape(1, 1, comps, writers, cap, LANES)


def solution(mesh):
    n_gx, n_gy, n_wa = mesh.shape["gx"], mesh.shape["gy"], mesh.shape["wa"]
    return jax.shard_map(
        functools.partial(local, n_gx, n_gy, n_wa),
        mesh=mesh,
        in_specs=(
            P(None, "gx", "gy", "wa"),
            P("gx", "gy", "wa", None),
            P("gx", "gy", "wa", None, None),
        ),
        out_specs=P(("gx", "gy"), "wa", None, None, None, None),
        check_vma=False,
    )
```

```python
import functools

import jax
import jax.numpy as jnp
from jax import lax
from jax.experimental import pallas as pl
from jax.experimental.pallas import tpu as pltpu
from jax.sharding import PartitionSpec as P

BY = 8
BZ = 16
COMP = 3
LANES = 128
MESH = pl.DeviceIdType.MESH


def dct_table(count):
    freqs = jnp.arange(count, dtype=jnp.float32)[:, None]
    points = jnp.arange(count, dtype=jnp.float32)[None, :]
    table = jnp.cos(jnp.pi * (points + 0.5) * freqs / count) * jnp.sqrt(2.0 / count)
    return jnp.where(freqs == 0.0, table * jnp.sqrt(0.5), table)


def split(value):
    high = value.astype(jnp.bfloat16)
    low = (value - high.astype(jnp.float32)).astype(jnp.bfloat16)
    return high, low


def dot(a, b):
    return jnp.dot(a, b, preferred_element_type=jnp.float32)


def iota(shape, dim):
    return lax.broadcasted_iota(jnp.int32, shape, dim)


def turned_row(block):
    return block // 64 * 64 + block % 8 * 8 + block // 8 % 8


def make_table(writers, cap, dest_ref, lens_ref, slots_ref, keep_ref):
    groups = dest_ref.shape[0]
    nblk = groups * LANES
    square = (LANES, LANES)
    upper = (iota(square, 0) < iota(square, 1)).astype(jnp.bfloat16)
    diagonal = iota(square, 0) == turned_row(iota(square, 1))
    ones = jnp.ones(square, jnp.bfloat16)
    freqs = iota(square, 1).astype(jnp.float32)
    rows_w = iota((writers, LANES), 0)
    rows_s = iota((cap, LANES), 0).astype(jnp.float32)
    lane = iota((1, LANES), 1)
    count = jnp.zeros((writers, 1), jnp.float32)
    high = jnp.zeros((writers, cap), jnp.float32)
    low = jnp.zeros((writers, cap), jnp.float32)
    across = (((1,), (1,)), ((), ()))
    for group in range(groups):
        named = rows_w == dest_ref[pl.ds(group, 1), :]
        one = named.astype(jnp.float32)
        one_b = one.astype(jnp.bfloat16)
        before = dot(one_b, upper) + count
        rank = jnp.sum(one * before, axis=0, keepdims=True)
        at_slot = rows_s == rank
        number = turned_row(lane) + (group * LANES + 1)
        top = jnp.where(at_slot, (number // 64).astype(jnp.float32), 0.0).astype(jnp.bfloat16)
        rest = jnp.where(at_slot, (number % 64).astype(jnp.float32), 0.0).astype(jnp.bfloat16)
        high += lax.dot_general(one_b, top, across, preferred_element_type=jnp.float32)
        low += lax.dot_general(one_b, rest, across, preferred_element_type=jnp.float32)
        count += jnp.sum(one, axis=1, keepdims=True)
        lens = lens_ref[pl.ds(group, 1), :].astype(jnp.float32)
        spread = jnp.where(diagonal, jnp.broadcast_to(lens, square), 0.0).astype(jnp.bfloat16)
        keep_ref[pl.ds(group * LANES, LANES), :] = (freqs < dot(spread, ones)).astype(jnp.float32)
    code = (high * 64.0 + low).astype(jnp.int32)
    slots_ref[...] = jnp.clip(jnp.where(code == 0, nblk, code - 1), 0, nblk)


def make_packing(n_gx, n_gy, most, dest_ref, lens_ref, first_ref, second_ref, codes_ref, keep_ref):
    writers = n_gx * n_gy
    groups = dest_ref.shape[0]
    nblk = groups * LANES
    square = (LANES, LANES)
    upper = (iota(square, 0) < iota(square, 1)).astype(jnp.bfloat16)
    diagonal = iota(square, 0) == turned_row(iota(square, 1))
    ones = jnp.ones(square, jnp.bfloat16)
    freqs = iota(square, 1).astype(jnp.float32)
    rows_w = iota((writers, LANES), 0)
    rows_k = iota((2 * n_gy, LANES), 0)
    rows_s = iota(square, 0)
    rows_r = iota((most, LANES), 0)
    lane = iota((1, LANES), 1)
    f32, bf16 = jnp.float32, jnp.bfloat16
    across = (((1,), (1,)), ((), ()))
    count = jnp.zeros((writers, 1), f32)
    kinds = jnp.zeros((2 * n_gy, 1), f32)
    blocks_high = jnp.zeros((2 * n_gy, most), f32)
    blocks_low = jnp.zeros((2 * n_gy, most), f32)
    codes_high = jnp.zeros((writers, LANES), f32)
    codes_low = jnp.zeros((writers, LANES), f32)

    def numbers(where, number):
        high = jnp.where(where, (number // 64).astype(f32), 0.0).astype(bf16)
        low = jnp.where(where, (number % 64).astype(f32), 0.0).astype(bf16)
        return high, low

    def summed(a, b):
        return lax.dot_general(a, b, across, preferred_element_type=f32)

    for group in range(groups):
        dest = dest_ref[pl.ds(group, 1), :]
        lens = lens_ref[pl.ds(group, 1), :]
        plane = dest % n_gy
        short = jnp.where(lens <= LANES // 2, 1, 0)
        one = (rows_w == plane * n_gx + dest // n_gy).astype(f32)
        one_b = one.astype(bf16)
        slot = jnp.sum(one * (dot(one_b, upper) + count), axis=0, keepdims=True).astype(jnp.int32)
        count += jnp.sum(one, axis=1, keepdims=True)
        kind = (rows_k == plane + n_gy * short).astype(f32)
        place = jnp.sum(kind * (dot(kind.astype(bf16), upper) + kinds), axis=0, keepdims=True)
        place = place.astype(jnp.int32)
        kinds += jnp.sum(kind, axis=1, keepdims=True)
        half = short * (place % 2)
        row = jnp.where(short == 1, most - 1 - place // 2, place)
        chosen = (rows_k == plane + n_gy * half).astype(bf16)
        high, low = numbers(rows_r == row, turned_row(lane) + (group * LANES + 1))
        blocks_high += summed(chosen, high)
        blocks_low += summed(chosen, low)
        high, low = numbers(rows_s == slot, row + 1 + 1024 * (short + half))
        codes_high += summed(one_b, high)
        codes_low += summed(one_b, low)
        spread = jnp.where(diagonal, jnp.broadcast_to(lens.astype(f32), square), 0.0).astype(bf16)
        keep_ref[pl.ds(group * LANES, LANES), :] = (freqs < dot(spread, ones)).astype(f32)
    block = (blocks_high * 64.0 + blocks_low).astype(jnp.int32)
    block = jnp.clip(jnp.where(block == 0, nblk, block - 1), 0, nblk)
    first_ref[...] = block[:n_gy]
    second_ref[...] = block[n_gy:]
    code = (codes_high * 64.0 + codes_low).astype(jnp.int32)
    where = jnp.where(code == 0, 3 * most, code // 1024 * most + code % 1024 - 1)
    codes_ref[...] = jnp.clip(where, 0, 3 * most).reshape(n_gy, n_gx, LANES)
    return jnp.where(2.0 * kinds[:n_gy] + kinds[n_gy:] > 2.0 * most, 1.0, 0.0)


def exchange_kernel(
    sizes, field, dest, lens, table, result,
    x_in, y_out, y_in, z_out, z_in, turned, coeffs, rows, received, keep, slots_v, slots,
    part, parts, plane_sum, plane_sums,
    halo_send, halo_recv, row_send, row_recv, own_sem, out_sem, slot_sem,
    part_send, part_recv, sum_send, sum_recv,
):
    n_gx, n_gy, n_wa, cells_x, cells_y, nblk, cap = sizes
    writers = n_gx * n_gy
    tiles_y = cells_y // 8
    gx, gy, wa = lax.axis_index("gx"), lax.axis_index("gy"), lax.axis_index("wa")
    me = gx * n_gy + gy

    def writer(w):
        return (w // n_gy, lax.rem(w, n_gy), wa)

    barrier = pltpu.get_barrier_semaphore()

    def greet(i, carry):
        pl.semaphore_signal(
            barrier, inc=1, device_id=writer(lax.rem(me + i, writers)), device_id_type=MESH
        )
        return carry

    lax.fori_loop(1, writers, greet, 0)
    for k in range(1, n_wa):
        pl.semaphore_signal(
            barrier, inc=1, device_id=(gx, gy, lax.rem(wa + k, n_wa)), device_id_type=MESH
        )

    lane = iota((8, LANES), 1)
    sub = iota((8, LANES), 0)
    zero = jnp.zeros((8, LANES), jnp.float32)
    packs = cells_x * 8 // LANES
    per = cells_x // packs

    def tile(c, x, y):
        return field[c, pl.ds(x * cells_y + y, tiles_y, stride=8), :]

    def pack_y(c, j):
        def pack(x, carry):
            y_out[0, j, pl.ds(x, 1), :] = field[c, pl.ds(x * cells_y, 1), :]
            y_out[1, j, pl.ds(x, 1), :] = field[c, pl.ds((x + 1) * cells_y - 1, 1), :]
            return carry

        lax.fori_loop(0, cells_x, pack, 0)

    def pack_z(c, j):
        for g in range(packs):

            def pack(step, carry):
                low, high = carry
                for x, y in [(x, y) for x in range(2) for y in range(8)]:
                    k = (step * 2 + x) * 8 + y
                    here = tile(c, g * per + step * 2 + x, y)
                    low = jnp.where(lane == k, pltpu.roll(here, k, 1), low)
                    high = jnp.where(lane == k, pltpu.roll(here, lax.rem(k + 1, LANES), 1), high)
                return low, high

            low, high = lax.fori_loop(0, per // 2, pack, (zero, zero))
            z_out[0, j, g] = low
            z_out[1, j, g] = high

    x_up = (lax.rem(gx + 1, n_gx), gy, wa)
    x_down = (lax.rem(gx + n_gx - 1, n_gx), gy, wa)
    y_up = (gx, lax.rem(gy + 1, n_gy), wa)
    y_down = (gx, lax.rem(gy + n_gy - 1, n_gy), wa)
    z_up = (gx, gy, lax.rem(wa + 1, n_wa))
    z_down = (gx, gy, lax.rem(wa + n_wa - 1, n_wa))
    faces = [
        (z_out.at[0, 1], z_in.at[0, 1], z_down),
        (z_out.at[1, 1], z_in.at[1, 1], z_up),
        (y_out.at[0, 1], y_in.at[0, 1], y_down),
        (y_out.at[1, 1], y_in.at[1, 1], y_up),
        (z_out.at[0, 0], z_in.at[0, 0], z_down),
        (z_out.at[1, 0], z_in.at[1, 0], z_up),
        (y_out.at[0, 0], y_in.at[0, 0], y_down),
        (y_out.at[1, 0], y_in.at[1, 0], y_up),
        (field.at[pl.ds(1, 2), pl.ds(0, cells_y)], x_in.at[0], x_down),
        (field.at[pl.ds(1, 2), pl.ds((cells_x - 1) * cells_y, cells_y)], x_in.at[1], x_up),
    ]
    halos = [
        pltpu.make_async_remote_copy(
            src_ref=source, dst_ref=target, send_sem=halo_send.at[k], recv_sem=halo_recv.at[k],
            device_id=peer, device_id_type=MESH,
        )
        for k, (source, target, peer) in enumerate(faces)
    ]

    pack_z(1, 1)
    pack_y(2, 1)
    pack_z(0, 0)
    pack_y(0, 0)
    make_table(writers, cap, dest, lens, slots_v, keep)
    slot_copy = pltpu.make_async_copy(slots_v, slots, slot_sem)
    slot_copy.start()
    pl.semaphore_wait(barrier, writers - 1 + n_wa - 1)
    for halo in halos:
        halo.start()
    coeffs[pl.ds(nblk, 8), :] = zero

    group = lane // BZ

    def turn(tiles):
        for step in (4, 2, 1):
            bit = (group // step) % 2 == 1
            out = list(tiles)
            for a in range(8):
                if a & step == 0:
                    b = a | step
                    out[a] = jnp.where(bit, pltpu.roll(tiles[b], BZ * step, 1), tiles[a])
                    out[b] = jnp.where(bit, tiles[b], pltpu.roll(tiles[a], LANES - BZ * step, 1))
            tiles = out
        return tiles

    def along_x(c, x, edge):
        def near(at, d):
            if edge == d:
                return [x_in[d, c - 1, pl.ds(y, tiles_y, stride=8), :] for y in range(8)]
            return [tile(c, at, y) for y in range(8)]

        return [a - b for a, b in zip(near(x + 1, 0), near(x - 1, 1))]

    def along_y(c, j, x):
        here = [tile(c, x, y) for y in range(8)]
        after = jnp.where(sub == tiles_y - 1, y_in[0, j, pl.ds(x, 1), :], pltpu.roll(here[0], tiles_y - 1, 0))
        before = jnp.where(sub == 0, y_in[1, j, pl.ds(x, 1), :], pltpu.roll(here[7], 1, 0))
        return [a - b for a, b in zip(here[1:] + [after], [before] + here[:-1])]

    def along_z(c, j, x):
        nexts, lasts = z_in[0, j, x // per], z_in[1, j, x // per]
        out = []
        for y in range(8):
            k = lax.rem(x, per) * 8 + y
            here = tile(c, x, y)
            after = jnp.where(
                lane == LANES - 1, pltpu.roll(nexts, LANES - 1 - k, 1), pltpu.roll(here, LANES - 1, 1)
            )
            before = jnp.where(
                lane == 0, pltpu.roll(lasts, lax.rem(LANES - k, LANES), 1), pltpu.roll(here, 1, 1)
            )
            out.append(after - before)
        return out

    def curl(c, square):
        def at(x, square, edge=None):
            if c == 0:
                pairs = zip(along_y(2, 1, x), along_z(1, 1, x))
            elif c == 1:
                pairs = zip(along_z(0, 0, x), along_x(2, x, edge))
            else:
                pairs = zip(along_x(1, x, edge), along_y(0, 0, x))
            tiles = [(a - b) * 0.5 for a, b in pairs]
            for t in tiles:
                square += t * t
            for z, t in enumerate(turn(tiles)):
                turned[c, pl.ds(x * cells_y + z * tiles_y, tiles_y), :] = t
            return square

        if c == 0:
            return lax.fori_loop(0, cells_x // 2, lambda i, q: at(2 * i + 1, at(2 * i, q)), square)
        square = at(0, square, 1)
        square = lax.fori_loop(1, cells_x - 1, at, square)
        return at(cells_x - 1, square, 0)

    chunk = 2 * LANES

    def row_copy(c, i, slot):
        peer = lax.rem(me + i, writers)
        return pltpu.make_async_remote_copy(
            src_ref=rows.at[c, peer], dst_ref=received.at[c, slot], send_sem=row_send.at[c, i],
            recv_sem=row_recv.at[c, i], device_id=writer(peer), device_id_type=MESH,
        )

    def own_copy(c):
        return pltpu.make_async_copy(rows.at[c, me], received.at[c, me], own_sem.at[c])

    def deliver(c):
        def transform(k, carry):
            at = pl.ds(k * chunk, chunk)
            high, low = split(turned[c, at, :])
            value = dot(high, table[0]) + (dot(low, table[0]) + dot(high, table[1]))
            coeffs[at, :] = value * keep[at, :]
            return carry

        lax.fori_loop(0, nblk // chunk, transform, 0)

        def gather(i):
            w = lax.rem(me + i, writers)
            for s in range(cap):
                rows[c, w, pl.ds(s, 1), :] = coeffs[pl.ds(slots[w, s], 1), :]

        gather(1)

        def step(i, carry):
            gather(i)
            row_copy(c, i - 1, me).start()
            return carry

        lax.fori_loop(2, writers, step, 0)
        gather(0)
        row_copy(c, writers - 1, me).start()
        own_copy(c).start()

    def part_copy(i, slot):
        return pltpu.make_async_remote_copy(
            src_ref=part, dst_ref=parts.at[slot], send_sem=part_send.at[i],
            recv_sem=part_recv.at[i], device_id=writer(lax.rem(me + i, writers)),
            device_id_type=MESH,
        )

    def sum_copy(k, slot):
        return pltpu.make_async_remote_copy(
            src_ref=plane_sum, dst_ref=plane_sums.at[slot], send_sem=sum_send.at[k],
            recv_sem=sum_recv.at[k], device_id=(gx, gy, lax.rem(wa + k, n_wa)),
            device_id_type=MESH,
        )

    for halo in halos[:4]:
        halo.wait()
    square = curl(0, zero)
    slot_copy.wait()
    deliver(0)
    for halo in halos[4:]:
        halo.wait()
    square = curl(2, curl(1, square))
    part[...] = square
    parts[pl.ds(me, 1)] = part[...][None]

    def part_start(i, carry):
        part_copy(i, me).start()
        return carry

    lax.fori_loop(1, writers, part_start, 0)
    deliver(1)
    deliver(2)

    def part_wait(i, carry):
        part_copy(i, lax.rem(me + writers - i, writers)).wait()
        return carry

    lax.fori_loop(1, writers, part_wait, 0)
    plane_sum[...] = jnp.sum(parts[...], axis=0)
    plane_sums[pl.ds(wa, 1)] = plane_sum[...][None]
    for k in range(1, n_wa):
        sum_copy(k, wa).start()
    for k in range(1, n_wa):
        sum_copy(k, lax.rem(wa + n_wa - k, n_wa)).wait()
    total = jnp.sum(plane_sums[...], axis=0)
    total = jnp.sum(jnp.sum(total, axis=0, keepdims=True), axis=1, keepdims=True)
    every = COMP * cells_x * cells_y * LANES * writers * n_wa
    scale = 1.0 / jnp.sqrt(total / every + 1e-06)
    scale = jnp.broadcast_to(jnp.broadcast_to(scale, (1, LANES)), (cap, LANES))

    for c in range(COMP):
        own_copy(c).wait()

        def row_wait(i, carry):
            row_copy(c, i, lax.rem(me + writers - i, writers)).wait()
            return carry

        lax.fori_loop(1, writers, row_wait, 0)

        def rescale(s, carry):
            received[c, s] = received[c, s] * scale
            return carry

        lax.fori_loop(0, writers, rescale, 0)
        pltpu.make_async_copy(received.at[c], result.at[c], out_sem.at[c]).start()
    for c in range(COMP):
        pltpu.make_async_copy(received.at[c], result.at[c], out_sem.at[c]).wait()


def relay_kernel(
    sizes, field, dest, lens, table, result, flag,
    x_in, y_out, y_in, z_out, z_in, turned, coeffs, shifted, packed, landed, spread, rows, received, keep,
    first_v, second_v, first, second, codes_out, codes_in, codes,
    part, parts, plane_sum, plane_sums,
    halo_send, halo_recv, row_send, row_recv, own_sem, out_sem, slot_sem,
    pack_send, pack_recv, code_send, code_recv,
    part_send, part_recv, sum_send, sum_recv,
):
    n_gx, n_gy, n_wa, cells_x, cells_y, nblk, cap, most = sizes
    writers = n_gx * n_gy
    tiles_y = cells_y // 8
    gx, gy, wa = lax.axis_index("gx"), lax.axis_index("gy"), lax.axis_index("wa")
    me = gx * n_gy + gy

    def writer(w):
        return (w // n_gy, lax.rem(w, n_gy), wa)

    barrier = pltpu.get_barrier_semaphore()

    def greet(i, carry):
        pl.semaphore_signal(
            barrier, inc=1, device_id=writer(lax.rem(me + i, writers)), device_id_type=MESH
        )
        return carry

    lax.fori_loop(1, writers, greet, 0)
    for k in range(1, n_wa):
        pl.semaphore_signal(
            barrier, inc=1, device_id=(gx, gy, lax.rem(wa + k, n_wa)), device_id_type=MESH
        )

    lane = iota((8, LANES), 1)
    sub = iota((8, LANES), 0)
    zero = jnp.zeros((8, LANES), jnp.float32)
    packs = cells_x * 8 // LANES
    per = cells_x // packs

    def tile(c, x, y):
        return field[c, pl.ds(x * cells_y + y, tiles_y, stride=8), :]

    def pack_y(c, j):
        def pack(x, carry):
            y_out[0, j, pl.ds(x, 1), :] = field[c, pl.ds(x * cells_y, 1), :]
            y_out[1, j, pl.ds(x, 1), :] = field[c, pl.ds((x + 1) * cells_y - 1, 1), :]
            return carry

        lax.fori_loop(0, cells_x, pack, 0)

    def pack_z(c, j):
        for g in range(packs):

            def pack(step, carry):
                low, high = carry
                for x, y in [(x, y) for x in range(2) for y in range(8)]:
                    k = (step * 2 + x) * 8 + y
                    here = tile(c, g * per + step * 2 + x, y)
                    low = jnp.where(lane == k, pltpu.roll(here, k, 1), low)
                    high = jnp.where(lane == k, pltpu.roll(here, lax.rem(k + 1, LANES), 1), high)
                return low, high

            low, high = lax.fori_loop(0, per // 2, pack, (zero, zero))
            z_out[0, j, g] = low
            z_out[1, j, g] = high

    x_up = (lax.rem(gx + 1, n_gx), gy, wa)
    x_down = (lax.rem(gx + n_gx - 1, n_gx), gy, wa)
    y_up = (gx, lax.rem(gy + 1, n_gy), wa)
    y_down = (gx, lax.rem(gy + n_gy - 1, n_gy), wa)
    z_up = (gx, gy, lax.rem(wa + 1, n_wa))
    z_down = (gx, gy, lax.rem(wa + n_wa - 1, n_wa))
    faces = [
        (z_out.at[0, 1], z_in.at[0, 1], z_down),
        (z_out.at[1, 1], z_in.at[1, 1], z_up),
        (y_out.at[0, 1], y_in.at[0, 1], y_down),
        (y_out.at[1, 1], y_in.at[1, 1], y_up),
        (z_out.at[0, 0], z_in.at[0, 0], z_down),
        (z_out.at[1, 0], z_in.at[1, 0], z_up),
        (y_out.at[0, 0], y_in.at[0, 0], y_down),
        (y_out.at[1, 0], y_in.at[1, 0], y_up),
        (field.at[pl.ds(1, 2), pl.ds(0, cells_y)], x_in.at[0], x_down),
        (field.at[pl.ds(1, 2), pl.ds((cells_x - 1) * cells_y, cells_y)], x_in.at[1], x_up),
    ]
    halos = [
        pltpu.make_async_remote_copy(
            src_ref=source, dst_ref=target, send_sem=halo_send.at[k], recv_sem=halo_recv.at[k],
            device_id=peer, device_id_type=MESH,
        )
        for k, (source, target, peer) in enumerate(faces)
    ]

    pack_z(1, 1)
    pack_y(2, 1)
    pack_z(0, 0)
    pack_y(0, 0)
    over = make_packing(n_gx, n_gy, most, dest, lens, first_v, second_v, codes_out, keep)
    tables = [
        pltpu.make_async_copy(first_v, first, slot_sem.at[0]),
        pltpu.make_async_copy(second_v, second, slot_sem.at[1]),
    ]
    for copy in tables:
        copy.start()
    pl.semaphore_wait(barrier, writers - 1 + n_wa - 1)
    for halo in halos:
        halo.start()

    def offset(k):
        odd = lax.rem(k, 2)
        return lax.rem(odd * ((k + 1) // 2) + (1 - odd) * (n_gy - k // 2), n_gy)

    def plane_to(k):
        return lax.rem(gy + offset(k), n_gy)

    def plane_from(k):
        return lax.rem(gy + n_gy - offset(k), n_gy)

    def code_copy(k, slot):
        return pltpu.make_async_remote_copy(
            src_ref=codes_out.at[plane_to(k)], dst_ref=codes_in.at[slot], send_sem=code_send.at[k],
            recv_sem=code_recv.at[k], device_id=(gx, plane_to(k), wa), device_id_type=MESH,
        )

    for k in range(1, n_gy):
        code_copy(k, gy).start()
    codes_in[pl.ds(gy, 1)] = codes_out[pl.ds(gy, 1)]
    coeffs[pl.ds(nblk, 8), :] = zero
    shifted[pl.ds(nblk, 8), :] = zero
    spread[pl.ds(3 * most, 8), :] = zero

    group = lane // BZ

    def turn(tiles):
        for step in (4, 2, 1):
            bit = (group // step) % 2 == 1
            out = list(tiles)
            for a in range(8):
                if a & step == 0:
                    b = a | step
                    out[a] = jnp.where(bit, pltpu.roll(tiles[b], BZ * step, 1), tiles[a])
                    out[b] = jnp.where(bit, tiles[b], pltpu.roll(tiles[a], LANES - BZ * step, 1))
            tiles = out
        return tiles

    def along_x(c, x, edge):
        def near(at, d):
            if edge == d:
                return [x_in[d, c - 1, pl.ds(y, tiles_y, stride=8), :] for y in range(8)]
            return [tile(c, at, y) for y in range(8)]

        return [a - b for a, b in zip(near(x + 1, 0), near(x - 1, 1))]

    def along_y(c, j, x):
        here = [tile(c, x, y) for y in range(8)]
        after = jnp.where(sub == tiles_y - 1, y_in[0, j, pl.ds(x, 1), :], pltpu.roll(here[0], tiles_y - 1, 0))
        before = jnp.where(sub == 0, y_in[1, j, pl.ds(x, 1), :], pltpu.roll(here[7], 1, 0))
        return [a - b for a, b in zip(here[1:] + [after], [before] + here[:-1])]

    def along_z(c, j, x):
        nexts, lasts = z_in[0, j, x // per], z_in[1, j, x // per]
        out = []
        for y in range(8):
            k = lax.rem(x, per) * 8 + y
            here = tile(c, x, y)
            after = jnp.where(
                lane == LANES - 1, pltpu.roll(nexts, LANES - 1 - k, 1), pltpu.roll(here, LANES - 1, 1)
            )
            before = jnp.where(
                lane == 0, pltpu.roll(lasts, lax.rem(LANES - k, LANES), 1), pltpu.roll(here, 1, 1)
            )
            out.append(after - before)
        return out

    def curl(c, square):
        def at(x, square, edge=None):
            if c == 0:
                pairs = zip(along_y(2, 1, x), along_z(1, 1, x))
            elif c == 1:
                pairs = zip(along_z(0, 0, x), along_x(2, x, edge))
            else:
                pairs = zip(along_x(1, x, edge), along_y(0, 0, x))
            tiles = [(a - b) * 0.5 for a, b in pairs]
            for t in tiles:
                square += t * t
            for z, t in enumerate(turn(tiles)):
                turned[c, pl.ds(x * cells_y + z * tiles_y, tiles_y), :] = t
            return square

        if c == 0:
            return lax.fori_loop(0, cells_x // 2, lambda i, q: at(2 * i + 1, at(2 * i, q)), square)
        square = at(0, square, 1)
        square = lax.fori_loop(1, cells_x - 1, at, square)
        return at(cells_x - 1, square, 0)

    chunk = 2 * LANES

    def row_copy(c, k, e, slot):
        column = lax.rem(gx + e, n_gx)
        return pltpu.make_async_remote_copy(
            src_ref=rows.at[c, column, plane_from(k)], dst_ref=received.at[c, slot],
            send_sem=row_send.at[c, k, e], recv_sem=row_recv.at[c, k, e],
            device_id=(column, gy, wa), device_id_type=MESH,
        )

    def own_copy(c, k):
        plane = plane_from(k)
        return pltpu.make_async_copy(
            rows.at[c, gx, plane], received.at[c, gx * n_gy + plane], own_sem.at[c, k]
        )

    def pack_copy(c, k, slot):
        return pltpu.make_async_remote_copy(
            src_ref=packed.at[c, plane_to(k)], dst_ref=landed.at[c, slot],
            send_sem=pack_send.at[c, k], recv_sem=pack_recv.at[c, k],
            device_id=(gx, plane_to(k), wa), device_id_type=MESH,
        )

    def deliver(c):
        def transform(k, carry):
            at = pl.ds(k * chunk, chunk)
            high, low = split(turned[c, at, :])
            value = dot(high, table[0]) + (dot(low, table[0]) + dot(high, table[1]))
            value = value * keep[at, :]
            coeffs[at, :] = value
            shifted[at, :] = pltpu.roll(value, LANES // 2, 1)
            return carry

        lax.fori_loop(0, nblk // chunk, transform, 0)

        def fill(plane, q):
            for s in range(64):
                r = q * 64 + s
                packed[c, plane, pl.ds(r, 1), :] = (
                    coeffs[pl.ds(first[plane, r], 1), :] + shifted[pl.ds(second[plane, r], 1), :]
                )

        def rest(plane):
            lax.fori_loop(1, most // 64, lambda q, carry: (fill(plane, q), carry)[1], 0)

        fill(plane_to(1), 0)
        rest(plane_to(1))

        def step(k, carry):
            fill(plane_to(k), 0)
            pack_copy(c, k - 1, gy).start()
            rest(plane_to(k))
            return carry

        lax.fori_loop(2, n_gy, step, 0)
        fill(gy, 0)
        pack_copy(c, n_gy - 1, gy).start()
        rest(gy)

    column64 = iota((64, LANES), 1) < LANES // 2

    def pass_on(c, k, source):
        def ready(q, carry):
            full = source(q)
            spread[pl.ds(q * 64, 64), :] = full
            spread[pl.ds(most + q * 64, 64), :] = jnp.where(column64, full, 0.0)
            turned_half = pltpu.roll(full, LANES // 2, 1)
            spread[pl.ds(2 * most + q * 64, 64), :] = jnp.where(column64, turned_half, 0.0)
            return carry

        lax.fori_loop(0, most // 64, ready, 0)
        plane = plane_from(k)

        def gather(e):
            column = lax.rem(gx + e, n_gx)
            for s in range(cap):
                rows[c, column, plane, pl.ds(s, 1), :] = spread[pl.ds(codes[plane, column, s], 1), :]

        gather(1)

        def step(e, carry):
            gather(e)
            row_copy(c, k, e - 1, gx * n_gy + plane).start()
            return carry

        lax.fori_loop(2, n_gx, step, 0)
        gather(0)
        row_copy(c, k, n_gx - 1, gx * n_gy + plane).start()
        own_copy(c, k).start()

    def relay(c):
        pass_on(c, 0, lambda q: packed[c, gy, pl.ds(q * 64, 64), :])

        def step(k, carry):
            plane = plane_from(k)
            pack_copy(c, k, plane).wait()
            pass_on(c, k, lambda q: landed[c, plane, pl.ds(q * 64, 64), :])
            return carry

        lax.fori_loop(1, n_gy, step, 0)

    def part_copy(i, slot):
        return pltpu.make_async_remote_copy(
            src_ref=part, dst_ref=parts.at[slot], send_sem=part_send.at[i],
            recv_sem=part_recv.at[i], device_id=writer(lax.rem(me + i, writers)),
            device_id_type=MESH,
        )

    def sum_copy(k, slot):
        return pltpu.make_async_remote_copy(
            src_ref=plane_sum, dst_ref=plane_sums.at[slot], send_sem=sum_send.at[k],
            recv_sem=sum_recv.at[k], device_id=(gx, gy, lax.rem(wa + k, n_wa)),
            device_id_type=MESH,
        )

    for halo in halos[:4]:
        halo.wait()
    square = curl(0, zero)
    for copy in tables:
        copy.wait()
    deliver(0)
    for halo in halos[4:]:
        halo.wait()
    square = curl(2, curl(1, square))
    part[0] = square
    part[1] = jnp.broadcast_to(over, (8, LANES))
    parts[pl.ds(me, 1)] = part[...][None]

    def part_start(i, carry):
        part_copy(i, me).start()
        return carry

    lax.fori_loop(1, writers, part_start, 0)
    deliver(1)

    for k in range(1, n_gy):
        code_copy(k, plane_from(k)).wait()
    code_load = pltpu.make_async_copy(codes_in, codes, slot_sem.at[2])
    code_load.start()
    code_load.wait()
    relay(0)
    deliver(2)

    def part_wait(i, carry):
        part_copy(i, lax.rem(me + writers - i, writers)).wait()
        return carry

    lax.fori_loop(1, writers, part_wait, 0)
    plane_sum[...] = jnp.sum(parts[...], axis=0)
    plane_sums[pl.ds(wa, 1)] = plane_sum[...][None]
    for k in range(1, n_wa):
        sum_copy(k, wa).start()
    relay(1)
    for k in range(1, n_wa):
        sum_copy(k, lax.rem(wa + n_wa - k, n_wa)).wait()
    total = jnp.sum(plane_sums[...], axis=0)
    flag[...] = total[1]
    total = total[0]
    total = jnp.sum(jnp.sum(total, axis=0, keepdims=True), axis=1, keepdims=True)
    every = COMP * cells_x * cells_y * LANES * writers * n_wa
    scale = 1.0 / jnp.sqrt(total / every + 1e-06)
    scale = jnp.broadcast_to(jnp.broadcast_to(scale, (1, LANES)), (cap, LANES))

    def finish(c, slot):
        received[c, slot] = received[c, slot] * scale
        pltpu.make_async_copy(received.at[c, slot], result.at[c, slot], out_sem.at[c]).start()

    def take(c):
        def from_plane(k, carry):
            plane = plane_from(k)
            own_copy(c, k).wait()
            finish(c, gx * n_gy + plane)

            def from_column(e, carry):
                slot = lax.rem(gx + n_gx - e, n_gx) * n_gy + plane
                row_copy(c, k, e, slot).wait()
                finish(c, slot)
                return carry

            return lax.fori_loop(1, n_gx, from_column, carry)

        lax.fori_loop(0, n_gy, from_plane, 0)

    take(0)
    relay(2)
    take(1)
    take(2)
    for c in range(COMP):
        pltpu.make_async_copy(received.at[c], result.at[c], out_sem.at[c]).wait()


def local(n_gx, n_gy, n_wa, velocity, lengths, destinations):
    comps, cells_x, cells_y, cells_z = velocity.shape
    nblk = lengths.size
    writers = n_gx * n_gy
    cap = max(2, 2 * nblk // writers)
    whole = pl.BlockSpec(memory_space=pltpu.VMEM)
    exact = jnp.kron(dct_table(BY), dct_table(BZ)).T
    high = lax.reduce_precision(exact, 8, 7)
    table = jnp.stack([high, exact - high]).astype(jnp.bfloat16)
    sizes = (n_gx, n_gy, n_wa, cells_x, cells_y, nblk, cap)
    f32 = jnp.float32
    packs = cells_x * cells_y // 8 // LANES
    dma = pltpu.SemaphoreType.DMA
    operands = (
        velocity.reshape(comps, cells_x * cells_y, cells_z),
        destinations.reshape(nblk // LANES, LANES),
        lengths.reshape(nblk // LANES, LANES),
        table,
    )
    most = n_gx * cap * 3 // 4
    result_shape = jax.ShapeDtypeStruct((comps, writers, cap, LANES), f32)
    direct = pl.pallas_call(
        functools.partial(exchange_kernel, sizes),
        out_shape=jax.ShapeDtypeStruct((comps, writers, cap, LANES), f32),
        in_specs=[whole, whole, whole, whole],
        out_specs=pl.BlockSpec(memory_space=pl.ANY),
        scratch_shapes=[
            pltpu.VMEM((2, 2, cells_y, LANES), f32),
            pltpu.VMEM((2, 2, cells_x, LANES), f32),
            pltpu.VMEM((2, 2, cells_x, LANES), f32),
            pltpu.VMEM((2, 2, packs, 8, LANES), f32),
            pltpu.VMEM((2, 2, packs, 8, LANES), f32),
            pltpu.VMEM((comps, nblk, LANES), f32),
            pltpu.VMEM((nblk + 8, LANES), f32),
            pltpu.VMEM((comps, writers, cap, LANES), f32),
            pltpu.VMEM((comps, writers, cap, LANES), f32),
            pltpu.VMEM((nblk, LANES), f32),
            pltpu.VMEM((writers, cap), jnp.int32),
            pltpu.SMEM((writers, cap), jnp.int32),
            pltpu.VMEM((8, LANES), f32),
            pltpu.VMEM((writers, 8, LANES), f32),
            pltpu.VMEM((8, LANES), f32),
            pltpu.VMEM((n_wa, 8, LANES), f32),
            dma((10,)),
            dma((10,)),
            dma((comps, writers)),
            dma((comps, writers)),
            dma((comps,)),
            dma((comps,)),
            dma,
            dma((writers,)),
            dma((writers,)),
            dma((n_wa,)),
            dma((n_wa,)),
        ],
        compiler_params=pltpu.CompilerParams(
            collective_id=0, has_side_effects=True, vmem_limit_bytes=40 * 2**20
        ),
    )
    relay = pl.pallas_call(
        functools.partial(relay_kernel, sizes + (most,)),
        out_shape=(result_shape, jax.ShapeDtypeStruct((8, LANES), f32)),
        in_specs=[whole, whole, whole, whole],
        out_specs=(pl.BlockSpec(memory_space=pl.ANY), whole),
        scratch_shapes=[
            pltpu.VMEM((2, 2, cells_y, LANES), f32),
            pltpu.VMEM((2, 2, cells_x, LANES), f32),
            pltpu.VMEM((2, 2, cells_x, LANES), f32),
            pltpu.VMEM((2, 2, packs, 8, LANES), f32),
            pltpu.VMEM((2, 2, packs, 8, LANES), f32),
            pltpu.VMEM((comps, nblk, LANES), f32),
            pltpu.VMEM((nblk + 8, LANES), f32),
            pltpu.VMEM((nblk + 8, LANES), f32),
            pltpu.VMEM((comps, n_gy, most, LANES), f32),
            pltpu.VMEM((comps, n_gy, most, LANES), f32),
            pltpu.VMEM((3 * most + 8, LANES), f32),
            pltpu.VMEM((comps, n_gx, n_gy, cap, LANES), f32),
            pltpu.VMEM((comps, writers, cap, LANES), f32),
            pltpu.VMEM((nblk, LANES), f32),
            pltpu.VMEM((n_gy, most), jnp.int32),
            pltpu.VMEM((n_gy, most), jnp.int32),
            pltpu.SMEM((n_gy, most), jnp.int32),
            pltpu.SMEM((n_gy, most), jnp.int32),
            pltpu.VMEM((n_gy, n_gx, LANES), jnp.int32),
            pltpu.VMEM((n_gy, n_gx, LANES), jnp.int32),
            pltpu.SMEM((n_gy, n_gx, LANES), jnp.int32),
            pltpu.VMEM((2, 8, LANES), f32),
            pltpu.VMEM((writers, 2, 8, LANES), f32),
            pltpu.VMEM((2, 8, LANES), f32),
            pltpu.VMEM((n_wa, 2, 8, LANES), f32),
            dma((10,)),
            dma((10,)),
            dma((comps, n_gy, n_gx)),
            dma((comps, n_gy, n_gx)),
            dma((comps, n_gy)),
            dma((comps,)),
            dma((3,)),
            dma((comps, n_gy)),
            dma((comps, n_gy)),
            dma((n_gy,)),
            dma((n_gy,)),
            dma((writers,)),
            dma((writers,)),
            dma((n_wa,)),
            dma((n_wa,)),
        ],
        compiler_params=pltpu.CompilerParams(
            collective_id=1, has_side_effects=True, vmem_limit_bytes=46 * 2**20
        ),
    )
    result, flag = relay(*operands)
    result = lax.cond(jnp.sum(flag) > 0.0, lambda: direct(*operands), lambda: result)
    return result.reshape(1, 1, comps, writers, cap, LANES)


def solution(mesh):
    n_gx, n_gy, n_wa = mesh.shape["gx"], mesh.shape["gy"], mesh.shape["wa"]
    return jax.shard_map(
        functools.partial(local, n_gx, n_gy, n_wa),
        mesh=mesh,
        in_specs=(
            P(None, "gx", "gy", "wa"),
            P("gx", "gy", "wa", None),
            P("gx", "gy", "wa", None, None),
        ),
        out_specs=P(("gx", "gy"), "wa", None, None, None, None),
        check_vma=False,
    )
```
